32 devices in a mesh: chan: 16 (over z, x, core), rng: 2 (over y).
Axes of the slice: x: 2, y: 2, z: 4, core: 2. Of those that a mesh axis runs over, the one named last changes fastest.
Arguments:
- radar_cube: bfloat16 [2, 512, 64, 256], P(None, 'chan', None, 'rng'), may hold values from -31 to 31, as said below
- offsets: int32 [32], P('chan'), may hold values from 0 to 7
- train_index: int32 [128], P('rng'), may hold values from 0 to 127, as said below
- guard_mask: int32 [256], P('rng'), may hold values 0 or 1
- weights: bfloat16 [2, 32, 64, 96], P(None, 'chan'), may hold values from -0.625 to 0.625
Outputs:
- covariance: float32 [64, 32, 2, 9216], P('rng', 'chan')
- matched_stat: float32 [32, 64, 256], P('chan', None, 'rng')
- power_map: float32 [32, 64, 256], P('chan', None, 'rng')
The draws below stay inside these ranges and needn't reach their ends.
Inputs may be any that keep to these rules, and one draw needn't show every extreme that they name: `radar_cube`: samples are finite real numbers. `weights`: for every subarray and bin, at least one of the 96 complex weights is nonzero. `train_index`: each aligned block of 64 entries lists distinct gates of the matching block of 128 gates, counted from that block's first gate.
All inputs are finite; a program needn't handle non-finite values. No bound on the sum of `guard_mask` on one device may be relied on, other than what follows from the above.
Results may differ from the reference program's by a relative error of at most 0.0039.
Values may be sent and summed in bfloat16 or wider, within the bound.
No kernel may reach another device: no remote copies, remote signals or barrier semaphores. Data moves between devices by JAX's collectives and lax.ppermute only.
A program may use at most 128 MiB of HBM per device.

```python
import math
from functools import partial
import jax
import jax.numpy as jnp
from jax import lax

PULSES = 64
CH_DEV = 32
SUB_LEN = 32
SUB_DEV = 2
SPAN = 8
RG_DEV = 128
STEP = 16
DOF = 96
TRAIN_DEV = 64
CHANNELS = 512
NSUB = 32
GATES = 256
TRAIN = 128


def draw_radar_cube(key, part):
    first_key, second_key = jax.random.split(jax.random.fold_in(key, 11), 2)
    channel_pos = jnp.arange(CHANNELS, dtype=jnp.float32) / (CHANNELS - 1)
    rising = (3.0 ** channel_pos)[None, :, None, None]
    rough = jnp.exp(jax.random.uniform(second_key, (1, CHANNELS, 1, GATES), jnp.float32, -0.7, 0.7))
    base = jnp.clip(jax.random.normal(first_key, (2, CHANNELS, PULSES, GATES), jnp.float32), -4.0, 4.0)
    return (base * rising * rough).astype(jnp.bfloat16)


def draw_train_index(key, part):
    blocks = GATES // RG_DEV
    keys = jax.random.split(jax.random.fold_in(key, 23), blocks)
    chosen = jax.vmap(lambda each_key: jax.random.permutation(each_key, RG_DEV)[:TRAIN_DEV])(keys)
    return chosen.reshape(-1).astype(jnp.int32)


def touch_ends(drawn, rng, smallest, high):
    place = [jax.random.randint(jax.random.fold_in(rng, axis), (), 0, length) for axis, length in enumerate(drawn.shape)]
    widest = drawn.shape.index(max(drawn.shape))
    beside = place[:widest] + [(place[widest] + 1) % drawn.shape[widest]] + place[widest + 1:]
    return drawn.at[tuple(place)].set(smallest).at[tuple(beside)].set(high)


def levels(stream_key, dims, cuts, low, top_value):
    def one(axis_at, blocks):
        heights = jax.random.uniform(jax.random.fold_in(jax.random.fold_in(stream_key, 6), axis_at), (blocks,), jnp.float32, low / len(cuts), top_value / len(cuts))
        return jnp.repeat(jnp.exp(heights), dims[axis_at] // blocks).reshape((-1,) + (1,) * (len(dims) - axis_at - 1))

    factor_of = one(*cuts[0])
    for cut in cuts[1:]:
        factor_of = factor_of * one(*cut)
    return factor_of


def bell_draw(stream_key, dims, scale, bound, pieces=(), kind=jnp.bfloat16):
    entries = scale * jax.random.normal(stream_key, dims, jnp.float32)
    if pieces:
        entries = entries * levels(stream_key, dims, pieces, -0.22, 0.18)
    return jnp.clip(entries, -bound, bound).astype(kind)


def setup_inputs(seed: int = 0) -> dict:
    streams_of = jax.random.split(jax.random.key(seed), 6)
    radar_cube = draw_radar_cube(jax.random.fold_in(streams_of[5], 71), 0)
    offsets = touch_ends(jax.random.randint(streams_of[1], (NSUB,), 0, SPAN), jax.random.fold_in(streams_of[1], 1), 0, SPAN - 1).astype(jnp.int32)
    train_index = draw_train_index(jax.random.fold_in(streams_of[5], 71), 0)
    guard_mask = touch_ends((jax.random.randint(streams_of[3], (GATES,), 0, 4) < 3).astype(jnp.int32), jax.random.fold_in(streams_of[3], 1), 0, 1)
    weights = bell_draw(streams_of[4], (2, NSUB, PULSES, DOF), DOF ** -0.5, 0.625, ((1, 16),))
    return dict(radar_cube=radar_cube, offsets=offsets, train_index=train_index, guard_mask=guard_mask, weights=weights)


diag_load = 1.0
highest = lax.Precision.HIGHEST

def dft_table(pulses):
    freq = jnp.arange(pulses, dtype=jnp.int32)
    phase = freq[:, None] * freq[None, :] % pulses
    angle = phase.astype(jnp.float32) * (2.0 * math.pi / pulses)
    cosine = jnp.cos(angle) / math.sqrt(pulses)
    sine = jnp.sin(angle) / math.sqrt(pulses)
    upper = jnp.stack([cosine, sine], axis=1)
    lower = jnp.stack([-sine, cosine], axis=1)
    return jnp.stack([upper, lower], axis=0).astype(jnp.bfloat16)

def one_window(radar_cube, train_index, guard_mask, weights, dft_mat, item):
    subarray, window_offset = item
    first = subarray // SUB_DEV * CH_DEV + subarray % SUB_DEV * STEP + window_offset
    channels = ((first + jnp.arange(SUB_LEN, dtype=jnp.int32)) % CHANNELS).astype(jnp.int32)
    raw_pulses = jnp.take(radar_cube, channels, axis=1).astype(jnp.float32)
    spectra = jnp.einsum('yqxp,xmpr->ymqr', dft_mat.astype(jnp.float32), raw_pulses, precision=highest)
    spectra = lax.optimization_barrier(spectra.astype(jnp.bfloat16)).astype(jnp.float32)
    snapshots = jnp.stack([jnp.roll(spectra, 1 - shift_bin, axis=2) for shift_bin in range(3)], axis=1)
    snapshots = snapshots.reshape(2, DOF, PULSES, GATES)
    snap_real = snapshots[0]
    snap_imag = snapshots[1]
    chosen = lax.dynamic_index_in_dim(weights, subarray, axis=1, keepdims=False).astype(jnp.float32)
    weight_real = chosen[0]
    weight_imag = chosen[1]
    out_real = jnp.einsum('kd,dkr->kr', weight_real, snap_real, precision=highest) + jnp.einsum('kd,dkr->kr', weight_imag, snap_imag, precision=highest)
    out_imag = jnp.einsum('kd,dkr->kr', weight_real, snap_imag, precision=highest) - jnp.einsum('kd,dkr->kr', weight_imag, snap_real, precision=highest)
    out_power = out_real * out_real + out_imag * out_imag
    gates = (jnp.arange(TRAIN, dtype=jnp.int32) // TRAIN_DEV * RG_DEV + train_index).astype(jnp.int32)
    keep = jnp.take(guard_mask, gates).astype(jnp.float32)
    picked = jnp.take(snapshots, gates, axis=3) * keep
    pick_real = picked[0]
    pick_imag = picked[1]
    cov_real = (jnp.einsum('ikt,jkt->kij', pick_real, pick_real, precision=highest) + jnp.einsum('ikt,jkt->kij', pick_imag, pick_imag, precision=highest)) / TRAIN
    cov_imag = (jnp.einsum('ikt,jkt->kij', pick_imag, pick_real, precision=highest) - jnp.einsum('ikt,jkt->kij', pick_real, pick_imag, precision=highest)) / TRAIN
    prod_real = jnp.einsum('kij,kj->ki', cov_real, weight_real, precision=highest) - jnp.einsum('kij,kj->ki', cov_imag, weight_imag, precision=highest)
    prod_imag = jnp.einsum('kij,kj->ki', cov_real, weight_imag, precision=highest) + jnp.einsum('kij,kj->ki', cov_imag, weight_real, precision=highest)
    quad_form = lax.optimization_barrier(jnp.sum(weight_real * prod_real + weight_imag * prod_imag, axis=-1)) + diag_load * lax.optimization_barrier(jnp.sum(weight_real * weight_real + weight_imag * weight_imag, axis=-1))
    matched = out_power / quad_form[:, None]
    covariance = jnp.stack([cov_real, cov_imag], axis=1).reshape(PULSES, 2, DOF * DOF)
    return (covariance, matched, out_power)

def reference(radar_cube, offsets, train_index, guard_mask, weights):
    dft_mat = dft_table(PULSES)
    items = (jnp.arange(NSUB, dtype=jnp.int32), offsets.astype(jnp.int32))
    covs, matched_stat, out_power = lax.map(partial(one_window, radar_cube, train_index, guard_mask, weights, dft_mat), items)
    covariance = jnp.transpose(covs, (1, 0, 2, 3))
    total_power = jnp.sum(out_power)
    mean_power = total_power / (NSUB * PULSES * GATES)
    power_map = out_power / (mean_power + 1e-06)
    return (covariance, matched_stat, power_map)
```

```python
import functools
import math

import jax
import jax.numpy as jnp
import numpy as np
from jax import lax
from jax.experimental import pallas as pl
from jax.experimental.pallas import tpu as pltpu
from jax.sharding import PartitionSpec as P

PULSES = 64
SUB_LEN = 32
SPAN = 8
DOF = 96
SHIFTS = DOF // SUB_LEN
LANES = 128
COV_CALLS = 2

diag_load = 1.0
f32 = jnp.float32
bf16 = jnp.bfloat16
VMEM = pl.BlockSpec(memory_space=pltpu.VMEM)
SMEM = pl.BlockSpec(memory_space=pltpu.SMEM)
BOTH = ("chan", "rng")


def params(mib, steps=0):
    semantics = ("arbitrary",) * steps if steps else None
    return pltpu.CompilerParams(vmem_limit_bytes=mib << 20, dimension_semantics=semantics)


def cost(flops, moved):
    return pl.CostEstimate(flops=int(flops), bytes_accessed=int(moved), transcendentals=0)


def dot(a, b):
    return jnp.dot(a, b, preferred_element_type=f32)


def dot_nt(a, b):
    return lax.dot_general(a, b, (((1,), (1,)), ((), ())), preferred_element_type=f32)


def dft_table(pulses):
    freq = np.arange(pulses)
    angle = 2.0 * math.pi * (freq[:, None] * freq[None, :] % pulses) / pulses
    cosine = np.cos(angle) / math.sqrt(pulses)
    sine = np.sin(angle) / math.sqrt(pulses)
    return np.block([[cosine, sine], [-sine, cosine]]).astype(np.float32)


def dft_kernel(table_ref, cube_ref, spec_ref, turned_re, turned_im):
    chans = cube_ref.shape[1]
    table = table_ref[...]
    for c in range(chans):
        block = jnp.concatenate([cube_ref[0, c], cube_ref[1, c]], axis=0)
        out = dot(table, block)
        turned_re[pl.ds(c, PULSES, stride=chans), :] = out[:PULSES]
        turned_im[pl.ds(c, PULSES, stride=chans), :] = out[PULSES:]
    gates = cube_ref.shape[3]
    spec_ref[:, :, :gates] = turned_re[...].astype(bf16).reshape(PULSES, chans, gates)
    spec_ref[:, :, gates:] = turned_im[...].astype(bf16).reshape(PULSES, chans, gates)


def pick_kernel(halo, place_ref, index_ref, mask_ref, spec_ref, count_ref, *refs):
    n_rng = (len(refs) - 1) // 2
    full_refs, head_refs, picked = refs[:n_rng], refs[n_rng : 2 * n_rng], refs[-1]
    chans = spec_ref.shape[1]
    train = index_ref.shape[1]
    gates = mask_ref.shape[1]
    half = PULSES // n_rng
    index = jnp.concatenate([index_ref[...], index_ref[...]], axis=1)
    row = lax.broadcasted_iota(jnp.int32, (2 * gates, 2 * train), 0)
    lane = lax.broadcasted_iota(jnp.int32, (2 * gates, 2 * train), 1)
    hit = (lax.rem(row, gates) == index) & ((row >= gates) == (lane >= train))
    select = jnp.where(hit, 1.0, 0.0).astype(bf16)
    mask = mask_ref[...].astype(f32).astype(bf16)
    mask = jnp.broadcast_to(jnp.concatenate([mask, mask], axis=1), (16, 2 * gates))
    keep = dot(mask, select)[:1]
    select = (select.astype(f32) * keep).astype(bf16)
    count_ref[...] = dot_nt(jnp.ones((8, 2 * train), bf16), select)[:, :gates]
    samples = spec_ref[...].reshape(PULSES * chans, 2 * gates)
    picked[...] = dot(samples, select).astype(bf16).reshape(PULSES, chans, 2 * train)
    for d in range(n_rng):
        owner = lax.rem(place_ref[0] + d, n_rng)

        def move(i, carry, d=d, owner=owner):
            found = picked[lax.rem(owner * half - 1 + i + PULSES, PULSES)]
            full_refs[d][i] = found
            head_refs[d][i] = found[:halo]
            return carry

        lax.fori_loop(0, half + 2, move, 0)


def filter_kernel(off_ref, w_ref, spec_ref, own_ref, prev_ref, banded):
    subs = w_ref.shape[2]
    chans = spec_ref.shape[1]
    gates = spec_ref.shape[2] // 2
    step = chans // subs
    per = LANES // chans
    lane = lax.broadcasted_iota(jnp.int32, (DOF, LANES), 1) & (chans - 1)
    dof = lax.broadcasted_iota(jnp.int32, (DOF, LANES), 0)
    bin_of = lax.broadcasted_iota(jnp.int32, (16, LANES), 0)
    near = lax.broadcasted_iota(jnp.int32, (16, LANES), 1) // chans - bin_of
    chunks = PULSES // per
    group = 0
    for src in range(2):
        for s in range(subs):
            start = src * chans - (s * step + off_ref[src, s])
            place = lane + start
            inside = (place >= 0) & (place < SUB_LEN)
            moves = [
                jnp.where(inside & (place + b * SUB_LEN == dof), 1.0, 0.0).astype(bf16)
                for b in range(SHIFTS)
            ]
            moves = jnp.concatenate(moves, axis=1)
            for part in range(2):
                spread = dot(w_ref[src, part, s], moves)
                for block in range(PULSES // 16):
                    rows = slice(block * 16, block * 16 + 16)
                    dst = pl.ds((group * 2 + part) * PULSES + block * 16, 16)
                    for j in range(chunks):
                        cols = slice(j * LANES, (j + 1) * LANES)
                        base = j * per - block * 16
                        reach = [(base + k - q) % PULSES for k in range(per) for q in range(16)]
                        if not any(t in (0, 1, PULSES - 1) for t in reach):
                            banded[dst, cols] = jnp.zeros((16, LANES), bf16)
                            continue
                        gap = (near + (base + PULSES)) & (PULSES - 1)
                        value = jnp.where(gap == 0, spread[rows, LANES : 2 * LANES], 0.0)
                        value = jnp.where(gap == PULSES - 1, spread[rows, :LANES], value)
                        value = jnp.where(gap == 1, spread[rows, 2 * LANES :], value)
                        banded[dst, cols] = value.astype(bf16)
            group += 1
    sums = dot(banded[...], spec_ref[...].reshape(PULSES * chans, 2 * gates))
    group = 0
    for out_ref in (own_ref, prev_ref):
        for s in range(subs):
            real = sums[group * 2 * PULSES : (group * 2 + 1) * PULSES]
            imag = sums[(group * 2 + 1) * PULSES : (group * 2 + 2) * PULSES]
            out_ref[s, 0] = real[:, :gates] + imag[:, gates:]
            out_ref[s, 1] = real[:, gates:] - imag[:, :gates]
            group += 1


def diagonal(rows):
    return lax.broadcasted_iota(jnp.int32, (rows, LANES), 0) == (
        lax.broadcasted_iota(jnp.int32, (rows, LANES), 1) & (rows - 1)
    )


def power_kernel(train_total, own_ref, other_ref, count_ref, power_ref, stats_ref):
    subs = own_ref.shape[0]
    count = count_ref[:1] / train_total
    total = jnp.zeros((1, LANES), f32)
    quad = jnp.zeros((1, LANES), f32)
    where_sub = lax.broadcasted_iota(jnp.int32, (PULSES, LANES), 1) // PULSES
    eye = diagonal(PULSES)
    for s in range(subs):
        real = own_ref[s, 0] + other_ref[s, 0]
        imag = own_ref[s, 1] + other_ref[s, 1]
        power = real * real + imag * imag
        power_ref[s] = power
        total = total + jnp.sum(power, axis=0, keepdims=True)
        column = jnp.sum(power * count, axis=1, keepdims=True)
        quad = quad + jnp.sum(jnp.where(eye & (where_sub == s), column, 0.0), axis=0, keepdims=True)
    total = jnp.broadcast_to(jnp.sum(total, axis=1, keepdims=True), (1, LANES))
    stats_ref[...] = jnp.concatenate([quad, total, jnp.zeros((6, LANES), f32)], axis=0)


def final_kernel(count, power_ref, w_ref, quad_ref, total_ref, matched_ref, map_ref):
    subs = power_ref.shape[0]
    mean = total_ref[1:2] / count
    where_sub = lax.broadcasted_iota(jnp.int32, (PULSES, LANES), 1) // PULSES
    eye = diagonal(PULSES)
    for s in range(subs):
        power = power_ref[s]
        pick = jnp.where(eye & (where_sub == s), quad_ref[:1], 0.0)
        quad = jnp.sum(pick, axis=1, keepdims=True)
        real = w_ref[0, s].astype(f32)
        imag = w_ref[1, s].astype(f32)
        norm = jnp.sum(real * real + imag * imag, axis=1, keepdims=True)
        matched_ref[s] = power / (quad + diag_load * norm)
        map_ref[s] = power / (mean + 1e-06)


def cov_kernel(first, train_total, step, n_rng, off_ref, *refs):
    full_refs, head_refs = refs[:n_rng], refs[n_rng : 2 * n_rng]
    out_ref, rows_scr, nat, perm = refs[-4:]
    per_step, subs = out_ref.shape[0], out_ref.shape[1]
    chans, halo = full_refs[0].shape[1], head_refs[0].shape[1]
    span = chans + halo
    pid = pl.program_id(0)
    sign = jnp.where(
        lax.broadcasted_iota(jnp.int32, (SUB_LEN, LANES), 1) < LANES // 2, 1.0, -1.0
    )

    def prepare(i):
        for d in range(n_rng):
            at = pl.multiple_of(i * span, 8)
            rows_scr[d, pl.ds(at, chans), :] = full_refs[d][first + i].astype(f32)
            rows_scr[d, pl.ds(at + chans, halo), :] = head_refs[d][first + i].astype(f32)
        for s in range(subs):
            base = i * span + s * step + off_ref[s]
            for d in range(n_rng):
                cols = slice(d * LANES, (d + 1) * LANES)
                nat[s, i, :, cols] = rows_scr[d, pl.ds(base, SUB_LEN), :].astype(bf16)
                parts = [rows_scr[d, pl.ds(base + k, SUB_LEN // 4, stride=4), :] for k in range(4)]
                mixed = jnp.concatenate(parts, axis=0)
                perm[s, i, 0, :, cols] = mixed.astype(bf16)
                perm[s, i, 1, :, cols] = (pltpu.roll(mixed, LANES // 2, 1) * sign).astype(bf16)

    @pl.when(pid == 0)
    def _():
        prepare(0)
        prepare(1)

    lane = lax.broadcasted_iota(jnp.int32, (8, LANES), 1)
    for g in range(per_step):
        k = pid * per_step + g
        prepare(k + 2)
        for s in range(subs):
            base = nat[s, pl.ds(k, SHIFTS)].reshape(DOF, n_rng * LANES)
            right = jnp.concatenate([base, base[: LANES - DOF]], axis=0)
            left = perm[s, pl.ds(k, SHIFTS)].reshape(2 * DOF, n_rng * LANES)
            prod = dot_nt(left, right) * (1.0 / train_total)
            for b in range(SHIFTS):
                for c in range(2):
                    at = (b * 2 + c) * SUB_LEN
                    m0, m1, m2, m3 = (prod[at + 8 * e : at + 8 * e + 8] for e in range(4))
                    m1r = pltpu.roll(m1, 96, 1)
                    m2r = pltpu.roll(m2, 64, 1)
                    m3r = pltpu.roll(m3, 32, 1)
                    rows = (
                        jnp.where(lane < 96, m0, m1),
                        jnp.where(lane < 64, m1r, m2r),
                        jnp.where(lane < 32, m2r, m3r),
                    )
                    for e in range(3):
                        out_ref[g, s, pl.ds(48 * b + 2 * e + c, 8, stride=6), :] = rows[e]


def local(radar_cube, offsets, train_index, guard_mask, weights):
    n_rng = lax.axis_size("rng")
    n_chan = lax.axis_size("chan")
    subs = offsets.shape[0]
    chans, gates = radar_cube.shape[1], radar_cube.shape[3]
    train = train_index.shape[0]
    step = chans // subs
    need = (subs - 1) * step + SPAN + SUB_LEN - 1 - chans
    halo = -(-need // 8) * 8
    half = PULSES // n_rng
    train_total = train * n_rng
    samples = 2 * train

    def send(x, by_chan, by_rng):
        pairs = [
            (c * n_rng + r, (c + by_chan) % n_chan * n_rng + (r + by_rng) % n_rng)
            for c in range(n_chan)
            for r in range(n_rng)
        ]
        return lax.ppermute(x, BOTH, pairs)

    prev_weights = send(weights, 1, 0)
    packed = jnp.broadcast_to(offsets.astype(f32)[:, None], (subs, LANES))
    prev_offsets = send(packed, 1, 0)[:, 0].astype(jnp.int32)

    spec = pl.pallas_call(
        dft_kernel,
        out_shape=jax.ShapeDtypeStruct((PULSES, chans, 2 * gates), bf16),
        in_specs=[VMEM, VMEM],
        out_specs=VMEM,
        scratch_shapes=[pltpu.VMEM((PULSES * chans, gates), f32)] * 2,
        compiler_params=params(16),
        cost_estimate=cost(2 * 128 * 128 * 128 * chans, 4 << 20),
        name="dft",
    )(jnp.asarray(dft_table(PULSES), bf16), radar_cube)

    full_type = jax.ShapeDtypeStruct((half + 2, chans, samples), bf16)
    head_type = jax.ShapeDtypeStruct((half + 2, halo, samples), bf16)
    place = lax.axis_index("rng").astype(jnp.int32).reshape(1)
    count, *cut = pl.pallas_call(
        functools.partial(pick_kernel, halo),
        out_shape=[jax.ShapeDtypeStruct((8, gates), f32)] + [full_type] * n_rng + [head_type] * n_rng,
        in_specs=[SMEM, VMEM, VMEM, VMEM],
        out_specs=[VMEM] * (1 + 2 * n_rng),
        scratch_shapes=[pltpu.VMEM((PULSES, chans, samples), bf16)],
        compiler_params=params(16),
        cost_estimate=cost(2 * PULSES * chans * 2 * gates * samples, 3 << 20),
        name="pick",
    )(place, train_index.reshape(1, train), guard_mask.reshape(1, gates), spec)
    fulls, heads = cut[:n_rng], cut[n_rng:]

    both_weights = jnp.stack([weights, prev_weights])
    both_offsets = jnp.stack([offsets, prev_offsets])
    sums_type = jax.ShapeDtypeStruct((subs, 2, PULSES, gates), f32)
    own_sums, prev_sums = pl.pallas_call(
        filter_kernel,
        out_shape=[sums_type, sums_type],
        in_specs=[SMEM, VMEM, VMEM],
        out_specs=[VMEM, VMEM],
        scratch_shapes=[pltpu.VMEM((4 * subs * PULSES, PULSES * chans), bf16)],
        compiler_params=params(20),
        cost_estimate=cost(2 * 4 * subs * PULSES * PULSES * chans * 2 * gates, 4 << 20),
        name="filter",
    )(both_offsets, both_weights, spec)

    got_full = [fulls[0]] + [send(fulls[d], 0, d) for d in range(1, n_rng)]
    other_sums = send(prev_sums, -1, 0)
    got_head = [send(heads[d], -1, d) for d in range(n_rng)]

    power, stats = pl.pallas_call(
        functools.partial(power_kernel, float(train_total)),
        out_shape=[
            jax.ShapeDtypeStruct((subs, PULSES, gates), f32),
            jax.ShapeDtypeStruct((8, LANES), f32),
        ],
        in_specs=[VMEM] * 3,
        out_specs=[VMEM] * 2,
        compiler_params=params(8),
        cost_estimate=cost(1 << 20, 1 << 20),
        name="power",
    )(own_sums, other_sums, count)

    for d in range(1, n_rng):
        stats = stats + send(stats, 0, d)
    quad_stats = stats
    total_stats = stats
    width = 1
    while width < n_chan:
        group = min(4, n_chan // width)
        wide = width * group

        def trade(x, k, width=width, group=group, wide=wide):
            pairs = []
            for c in range(n_chan):
                low, mid, high = c % width, c // width % group, c // wide * wide
                to = high + (mid + k) % group * width + low
                pairs += [(c * n_rng + r, to * n_rng + r) for r in range(n_rng)]
            return lax.ppermute(x, BOTH, pairs)

        total_stats = total_stats + sum(trade(total_stats, k) for k in range(1, group))
        width = wide

    cov_type = jax.ShapeDtypeStruct((half, subs, 2 * DOF * DOF // LANES, LANES), f32)
    per_step = 4
    covariance = None
    for part in range(COV_CALLS):
        bins = half // COV_CALLS
        first = part * bins
        steps = bins // per_step
        args = [offsets, *got_full, *got_head]
        specs = [SMEM] + [VMEM] * (2 * n_rng)
        aliases = {}
        if covariance is not None:
            args.append(covariance)
            specs.append(pl.BlockSpec(memory_space=pl.ANY))
            aliases = {len(args) - 1: 0}
        covariance = pl.pallas_call(
            functools.partial(cov_kernel, first, float(train_total), step, n_rng),
            out_shape=cov_type,
            grid=(steps,),
            in_specs=specs,
            out_specs=pl.BlockSpec(
                (per_step,) + cov_type.shape[1:],
                lambda i, start=first // per_step: (start + i, 0, 0, 0),
            ),
            scratch_shapes=[
                pltpu.VMEM((n_rng, (bins + 2) * (chans + halo), LANES), f32),
                pltpu.VMEM((subs, bins + 2, SUB_LEN, n_rng * LANES), bf16),
                pltpu.VMEM((subs, bins + 2, 2, SUB_LEN, n_rng * LANES), bf16),
            ],
            input_output_aliases=aliases,
            compiler_params=params(20, 1),
            cost_estimate=cost(2 * bins * subs * 192 * 128 * 256, 4 << 20),
            name="cov",
        )(*args)
    rows = DOF * DOF // LANES
    covariance = covariance.reshape(half, subs, rows, 2, LANES)
    covariance = covariance.transpose(0, 1, 3, 2, 4).reshape(half, subs, 2, DOF * DOF)

    out_type = jax.ShapeDtypeStruct((subs, PULSES, gates), f32)
    matched_stat, power_map = pl.pallas_call(
        functools.partial(final_kernel, float(subs * n_chan * PULSES * gates * n_rng)),
        out_shape=[out_type, out_type],
        in_specs=[VMEM] * 4,
        out_specs=[VMEM] * 2,
        compiler_params=params(8),
        cost_estimate=cost(1 << 20, 1 << 20),
        name="final",
    )(power, weights, quad_stats, total_stats)
    return (covariance, matched_stat, power_map)


def solution(mesh):
    placed = (
        P(None, "chan", None, "rng"),
        P("chan"),
        P("rng"),
        P("rng"),
        P(None, "chan", None, None),
    )
    return jax.shard_map(
        local,
        mesh=mesh,
        in_specs=placed,
        out_specs=(P("rng", "chan", None, None), P("chan", None, "rng"), P("chan", None, "rng")),
        check_vma=False,
    )
```

```python
import functools
import math

import jax
import jax.numpy as jnp
import numpy as np
from jax import lax
from jax.experimental import pallas as pl
from jax.experimental.pallas import tpu as pltpu
from jax.sharding import PartitionSpec as P

PULSES = 64
SUB_LEN = 32
SPAN = 8
DOF = 96
SHIFTS = DOF // SUB_LEN
LANES = 128
COV_CALLS = 1

diag_load = 1.0
f32 = jnp.float32
bf16 = jnp.bfloat16
VMEM = pl.BlockSpec(memory_space=pltpu.VMEM)
SMEM = pl.BlockSpec(memory_space=pltpu.SMEM)
HBM = pl.BlockSpec(memory_space=pltpu.HBM)
ANY = pl.BlockSpec(memory_space=pl.ANY)
BOTH = ("chan", "rng")


def params(mib, steps=0):
    semantics = ("arbitrary",) * steps if steps else None
    return pltpu.CompilerParams(vmem_limit_bytes=mib << 20, dimension_semantics=semantics)


def cost(flops, moved):
    return pl.CostEstimate(flops=int(flops), bytes_accessed=int(moved), transcendentals=0)


def in_hbm(x):
    return pltpu.with_memory_space_constraint(x, pltpu.HBM)


def dot(a, b):
    return jnp.dot(a, b, preferred_element_type=f32)


def dot_nt(a, b):
    return lax.dot_general(a, b, (((1,), (1,)), ((), ())), preferred_element_type=f32)


def dft_table(pulses):
    freq = np.arange(pulses)
    angle = 2.0 * math.pi * (freq[:, None] * freq[None, :] % pulses) / pulses
    cosine = np.cos(angle) / math.sqrt(pulses)
    sine = np.sin(angle) / math.sqrt(pulses)
    return np.block([[cosine, sine], [-sine, cosine]]).astype(np.float32)


def spectra_kernel(table_hbm, cube_hbm, *refs):
    chunks = 4
    table_ref, cube_ref, turned_re, turned_im, sems = refs[-5:]
    staged = len(refs[:-5]) // 2
    small_hbm, spec_ref, small_refs = refs[:staged], refs[staged], refs[staged + 1 : -5]
    chans, gates = cube_ref.shape[1], cube_ref.shape[3]
    each = chans // chunks
    first = pltpu.make_async_copy(table_hbm, table_ref, sems.at[chunks])
    large = [
        pltpu.make_async_copy(
            cube_hbm.at[:, pl.ds(i * each, each)], cube_ref.at[:, pl.ds(i * each, each)], sems.at[i]
        )
        for i in range(chunks)
    ]
    small = [
        pltpu.make_async_copy(src, dst, sems.at[chunks + 1 + i])
        for i, (src, dst) in enumerate(zip(small_hbm, small_refs, strict=True))
    ]
    for copy in [first, *large, *small]:
        copy.start()
    first.wait()
    table = table_ref[...]
    for c in range(0, chans, 2):
        if c % each == 0:
            large[c // each].wait()
        pair = [jnp.concatenate([cube_ref[0, e], cube_ref[1, e]], axis=0) for e in (c, c + 1)]
        out = dot(table, jnp.concatenate(pair, axis=1))
        for e in range(2):
            at = pl.ds(c + e, PULSES, stride=chans)
            turned_re[at, :] = out[:PULSES, e * gates : (e + 1) * gates]
            turned_im[at, :] = out[PULSES:, e * gates : (e + 1) * gates]
    spec_ref[:, :, :gates] = turned_re[...].astype(bf16).reshape(PULSES, chans, gates)
    spec_ref[:, :, gates:] = turned_im[...].astype(bf16).reshape(PULSES, chans, gates)
    for copy in small:
        copy.wait()


def pick_kernel(halo, place_ref, index_ref, mask_ref, spec_ref, count_ref, *refs):
    refs, picked = refs[:-1], refs[-1]
    n_rng = len(refs) // 2
    full_refs, head_refs = refs[:n_rng], refs[n_rng:]
    chans, gates = spec_ref.shape[1], mask_ref.shape[1]
    train = index_ref.shape[1]
    half = PULSES // n_rng
    index = jnp.concatenate([index_ref[...], index_ref[...]], axis=1)
    row = lax.broadcasted_iota(jnp.int32, (2 * gates, 2 * train), 0)
    lane = lax.broadcasted_iota(jnp.int32, (2 * gates, 2 * train), 1)
    hit = (lax.rem(row, gates) == index) & ((row >= gates) == (lane >= train))
    select = jnp.where(hit, 1.0, 0.0).astype(bf16)
    mask = mask_ref[...].astype(f32).astype(bf16)
    mask = jnp.broadcast_to(jnp.concatenate([mask, mask], axis=1), (16, 2 * gates))
    keep = dot(mask, select)[:1]
    select = (select.astype(f32) * keep).astype(bf16)
    count_ref[...] = dot_nt(jnp.ones((8, 2 * train), bf16), select)[:, :gates]
    samples = spec_ref[...].reshape(PULSES * chans, 2 * gates)
    picked[...] = dot(samples, select).astype(bf16).reshape(PULSES, chans, 2 * train)
    for d in range(n_rng):
        owner = lax.rem(place_ref[0] + d, n_rng)

        def move(i, carry, d=d, owner=owner):
            found = picked[lax.rem(owner * half - 1 + i + PULSES, PULSES)]
            full_refs[d][i] = found
            head_refs[d][i] = found[:halo]
            return carry

        lax.fori_loop(0, half + 2, move, 0)


def filter_kernel(off_ref, prev_off_ref, w_ref, prev_w_ref, spec_ref, own_ref, prev_ref, banded):
    subs = w_ref.shape[1]
    chans = spec_ref.shape[1]
    gates = spec_ref.shape[2] // 2
    step = chans // subs
    per = LANES // chans
    lane = lax.broadcasted_iota(jnp.int32, (DOF, LANES), 1) & (chans - 1)
    dof = lax.broadcasted_iota(jnp.int32, (DOF, LANES), 0)
    bin_of = lax.broadcasted_iota(jnp.int32, (16, LANES), 0)
    near = lax.broadcasted_iota(jnp.int32, (16, LANES), 1) // chans - bin_of
    chunks = PULSES // per
    group = 0
    for src, (offs, taps) in enumerate(((off_ref, w_ref), (prev_off_ref, prev_w_ref))):
        for s in range(subs):
            start = src * chans - s * step - offs[:, s : s + 1]
            place = lane + start
            inside = (place >= 0) & (place < SUB_LEN)
            moves = [
                jnp.where(inside & (place + b * SUB_LEN == dof), 1.0, 0.0).astype(bf16)
                for b in range(SHIFTS)
            ]
            moves = jnp.concatenate(moves, axis=1)
            for part in range(2):
                spread = dot(taps[part, s], moves)
                for block in range(PULSES // 16):
                    rows = slice(block * 16, block * 16 + 16)
                    dst = pl.ds((group * 2 + part) * PULSES + block * 16, 16)
                    for j in range(chunks):
                        cols = slice(j * LANES, (j + 1) * LANES)
                        base = j * per - block * 16
                        reach = [(base + k - q) % PULSES for k in range(per) for q in range(16)]
                        if not any(t in (0, 1, PULSES - 1) for t in reach):
                            banded[dst, cols] = jnp.zeros((16, LANES), bf16)
                            continue
                        gap = (near + (base + PULSES)) & (PULSES - 1)
                        value = jnp.where(gap == 0, spread[rows, LANES : 2 * LANES], 0.0)
                        value = jnp.where(gap == PULSES - 1, spread[rows, :LANES], value)
                        value = jnp.where(gap == 1, spread[rows, 2 * LANES :], value)
                        banded[dst, cols] = value.astype(bf16)
            group += 1
    sums = dot(banded[...], spec_ref[...].reshape(PULSES * chans, 2 * gates))
    group = 0
    for out_ref in (own_ref, prev_ref):
        for s in range(subs):
            real = sums[group * 2 * PULSES : (group * 2 + 1) * PULSES]
            imag = sums[(group * 2 + 1) * PULSES : (group * 2 + 2) * PULSES]
            out_ref[s, 0] = real[:, :gates] + imag[:, gates:]
            out_ref[s, 1] = real[:, gates:] - imag[:, :gates]
            group += 1


def diagonal(rows):
    return lax.broadcasted_iota(jnp.int32, (rows, LANES), 0) == (
        lax.broadcasted_iota(jnp.int32, (rows, LANES), 1) & (rows - 1)
    )


def power_kernel(train_total, own_ref, other_ref, count_ref, power_ref, stats_ref):
    subs = own_ref.shape[0]
    count = count_ref[:1] / train_total
    total = jnp.zeros((1, LANES), f32)
    quad = jnp.zeros((1, LANES), f32)
    where_sub = lax.broadcasted_iota(jnp.int32, (PULSES, LANES), 1) // PULSES
    eye = diagonal(PULSES)
    for s in range(subs):
        real = own_ref[s, 0] + other_ref[s, 0]
        imag = own_ref[s, 1] + other_ref[s, 1]
        power = real * real + imag * imag
        power_ref[s] = power
        total = total + jnp.sum(power, axis=0, keepdims=True)
        column = jnp.sum(power * count, axis=1, keepdims=True)
        quad = quad + jnp.sum(jnp.where(eye & (where_sub == s), column, 0.0), axis=0, keepdims=True)
    total = jnp.broadcast_to(jnp.sum(total, axis=1, keepdims=True), (1, LANES))
    stats_ref[...] = jnp.broadcast_to(jnp.concatenate([quad, total], axis=0)[None], stats_ref.shape)


def final_kernel(count, n_rng, block_ref, power_ref, w_ref, stats_ref, matched_ref, map_ref):
    subs = power_ref.shape[0]
    mean = jnp.sum(stats_ref[...], axis=0)[1:2] / count
    shares = jnp.sum(stats_ref[pl.ds(block_ref[0] * n_rng, n_rng)], axis=0)[:1]
    where_sub = lax.broadcasted_iota(jnp.int32, (PULSES, LANES), 1) // PULSES
    eye = diagonal(PULSES)
    for s in range(subs):
        power = power_ref[s]
        pick = jnp.where(eye & (where_sub == s), shares, 0.0)
        quad = jnp.sum(pick, axis=1, keepdims=True)
        real = w_ref[0, s].astype(f32)
        imag = w_ref[1, s].astype(f32)
        norm = jnp.sum(real * real + imag * imag, axis=1, keepdims=True)
        matched_ref[s] = power / (quad + diag_load * norm)
        map_ref[s] = power / (mean + 1e-06)


def cov_kernel(first, train_total, step, n_rng, off_ref, *refs):
    full_refs, head_refs = refs[:n_rng], refs[n_rng : 2 * n_rng]
    out_hbm, rows_scr, nat, perm, out_buf, sems = refs[-6:]
    bins, subs = out_buf.shape[0], out_buf.shape[1]
    chans, halo = full_refs[0].shape[1], head_refs[0].shape[1]
    span = chans + halo
    sign = jnp.where(
        lax.broadcasted_iota(jnp.int32, (SUB_LEN, LANES), 1) < LANES // 2, 1.0, -1.0
    )

    def prepare(i):
        for d in range(n_rng):
            rows_scr[d, pl.ds(i * span, chans), :] = full_refs[d][first + i].astype(f32)
            rows_scr[d, pl.ds(i * span + chans, halo), :] = head_refs[d][first + i].astype(f32)
        for s in range(subs):
            base = i * span + s * step + off_ref[s]
            for d in range(n_rng):
                cols = slice(d * LANES, (d + 1) * LANES)
                nat[s, i, :, cols] = rows_scr[d, pl.ds(base, SUB_LEN), :].astype(bf16)
                parts = [rows_scr[d, pl.ds(base + k, SUB_LEN // 4, stride=4), :] for k in range(4)]
                mixed = jnp.concatenate(parts, axis=0)
                perm[s, i, 0, :, cols] = mixed.astype(bf16)
                perm[s, i, 1, :, cols] = (pltpu.roll(mixed, LANES // 2, 1) * sign).astype(bf16)

    def turn(x, amount):
        x = x[:, amount // 2 * LANES : (amount // 2 + 1) * LANES]
        return pltpu.roll(x, SUB_LEN, 1) if amount % 2 else x

    def write(k):
        return pltpu.make_async_copy(
            out_buf.at[pl.ds(k, 2)], out_hbm.at[pl.ds(first + k, 2)], sems.at[k // 2]
        )

    for i in range(SHIFTS - 1):
        prepare(i)
    lane = lax.broadcasted_iota(jnp.int32, (8, LANES), 1)
    for k in range(0, bins, 2):
        prepare(k + 2)
        prepare(k + 3)
        for s in range(subs):
            right = nat[s, k : k + SHIFTS + 1].reshape((SHIFTS + 1) * SUB_LEN, n_rng * LANES)
            right = jnp.concatenate([right, right[LANES // 2 :], right[: LANES // 2]], axis=0)
            left = perm[s, k : k + SHIFTS + 1].reshape((SHIFTS + 1) * 2 * SUB_LEN, n_rng * LANES)
            prod = dot_nt(left, right) * (1.0 / train_total)
            for g in range(2):
                for b in range(SHIFTS):
                    for c in range(2):
                        at = ((b + g) * 2 + c) * SUB_LEN
                        m0, m1, m2, m3 = (
                            turn(prod[at + 8 * e : at + 8 * e + 8], (4 - e - g) % 4) for e in range(4)
                        )
                        rows = (
                            jnp.where(lane < 96, m0, m1),
                            jnp.where(lane < 64, m1, m2),
                            jnp.where(lane < 32, m2, m3),
                        )
                        for e in range(3):
                            at = 48 * b + 2 * e + c
                            out_buf[k + g, s, pl.ds(at, 8, stride=6), :] = rows[e]
        write(k).start()
    for k in range(0, bins, 2):
        write(k).wait()


def cov_scratch(bins, chans, halo, subs, n_rng):
    return [
        pltpu.VMEM((n_rng, (bins + 2) * (chans + halo), LANES), f32),
        pltpu.VMEM((subs, bins + 2, SUB_LEN, n_rng * LANES), bf16),
        pltpu.VMEM((subs, bins + 2, 2, SUB_LEN, n_rng * LANES), bf16),
        pltpu.VMEM((bins, subs, 2 * DOF * DOF // LANES, LANES), f32),
        pltpu.SemaphoreType.DMA((bins // 2,)),
    ]


def local(radar_cube, offsets, train_index, guard_mask, weights):
    n_rng = lax.axis_size("rng")
    n_chan = lax.axis_size("chan")
    subs = offsets.shape[0]
    chans, gates = radar_cube.shape[1], radar_cube.shape[3]
    train = train_index.shape[0]
    step = chans // subs
    need = (subs - 1) * step + SPAN + SUB_LEN - 1 - chans
    halo = -(-need // 8) * 8
    half = PULSES // n_rng
    train_total = train * n_rng
    samples = 2 * train

    def send(x, by_chan, by_rng):
        pairs = [
            (c * n_rng + r, (c + by_chan) % n_chan * n_rng + (r + by_rng) % n_rng)
            for c in range(n_chan)
            for r in range(n_rng)
        ]
        return lax.ppermute(x, BOTH, pairs)

    prev_weights = send(weights, 1, 0)
    prev_offsets = send(offsets, 1, 0)

    small = [
        train_index.reshape(1, train),
        guard_mask.reshape(1, gates),
        weights,
        offsets.reshape(1, subs),
    ]
    spec, near_index, near_mask, near_weights, near_offsets = pl.pallas_call(
        spectra_kernel,
        out_shape=[jax.ShapeDtypeStruct((PULSES, chans, 2 * gates), bf16)]
        + [jax.ShapeDtypeStruct(x.shape, x.dtype) for x in small],
        in_specs=[HBM] * (2 + len(small)),
        out_specs=[VMEM] * (1 + len(small)),
        scratch_shapes=[
            pltpu.VMEM((2 * PULSES, 2 * PULSES), bf16),
            pltpu.VMEM(radar_cube.shape, bf16),
            pltpu.VMEM((PULSES * chans, gates), f32),
            pltpu.VMEM((PULSES * chans, gates), f32),
            pltpu.SemaphoreType.DMA((5 + len(small),)),
        ],
        compiler_params=params(20),
        cost_estimate=cost(4 * PULSES * PULSES * chans * 2 * gates, 4 << 20),
        name="spectra",
    )(in_hbm(jnp.asarray(dft_table(PULSES), bf16)), in_hbm(radar_cube), *(in_hbm(x) for x in small))

    sums_type = jax.ShapeDtypeStruct((subs, 2, PULSES, gates), f32)
    own_sums, prev_sums = pl.pallas_call(
        filter_kernel,
        out_shape=[sums_type, sums_type],
        in_specs=[VMEM] * 5,
        out_specs=[VMEM, VMEM],
        scratch_shapes=[pltpu.VMEM((4 * subs * PULSES, PULSES * chans), bf16)],
        compiler_params=params(20),
        cost_estimate=cost(2 * 4 * subs * PULSES * PULSES * chans * 2 * gates, 4 << 20),
        name="filter",
    )(near_offsets, prev_offsets.reshape(1, subs), near_weights, prev_weights, spec)

    other_sums = send(prev_sums, -1, 0)
    full_type = jax.ShapeDtypeStruct((half + 2, chans, samples), bf16)
    head_type = jax.ShapeDtypeStruct((half + 2, halo, samples), bf16)
    place = lax.axis_index("rng").astype(jnp.int32).reshape(1)
    block = lax.axis_index("chan").astype(jnp.int32).reshape(1)
    count, *cut = pl.pallas_call(
        functools.partial(pick_kernel, halo),
        out_shape=[jax.ShapeDtypeStruct((8, gates), f32)] + [full_type] * n_rng + [head_type] * n_rng,
        in_specs=[SMEM, VMEM, VMEM, VMEM],
        out_specs=[VMEM] * (1 + 2 * n_rng),
        scratch_shapes=[pltpu.VMEM((PULSES, chans, samples), bf16)],
        compiler_params=params(20),
        cost_estimate=cost(2 * PULSES * chans * 2 * gates * samples, 3 << 20),
        name="pick",
    )(place, near_index, near_mask, spec)
    fulls, heads = cut[:n_rng], cut[n_rng:]

    got_full = [fulls[0]]
    for d in range(1, n_rng):
        got_full.append(send(fulls[d], 0, d))

    got_head = []
    for d in range(n_rng):
        got_head.append(send(heads[d], -1, d))

    power, stats = pl.pallas_call(
        functools.partial(power_kernel, float(train_total)),
        out_shape=[
            jax.ShapeDtypeStruct((subs, PULSES, gates), f32),
            jax.ShapeDtypeStruct((n_chan * n_rng, 2, LANES), f32),
        ],
        in_specs=[VMEM] * 3,
        out_specs=[VMEM] * 2,
        compiler_params=params(8),
        cost_estimate=cost(1 << 20, 1 << 20),
        name="power",
    )(own_sums, other_sums, count)

    stats = lax.all_to_all(stats, BOTH, 0, 0, tiled=True)

    cov_type = jax.ShapeDtypeStruct((half, subs, 2 * DOF * DOF // LANES, LANES), f32)
    covariance, first = None, 0
    for part in range(COV_CALLS):
        bins = 2 * ((half // 2 * (part + 1)) // COV_CALLS) - first
        args = [near_offsets.reshape(subs), *got_full, *got_head]
        specs = [SMEM] + [VMEM] * (2 * n_rng)
        aliases = {}
        if covariance is not None:
            args.append(covariance)
            specs.append(ANY)
            aliases = {len(args) - 1: 0}
        covariance = pl.pallas_call(
            functools.partial(cov_kernel, first, float(train_total), step, n_rng),
            out_shape=cov_type,
            in_specs=specs,
            out_specs=ANY,
            scratch_shapes=cov_scratch(bins, chans, halo, subs, n_rng),
            input_output_aliases=aliases,
            compiler_params=params(20),
            cost_estimate=cost(2 * bins * subs * 192 * 128 * 256, bins * 160000),
            name="cov",
        )(*args)
        first += bins
    rows = DOF * DOF // LANES
    covariance = covariance.reshape(half, subs, rows, 2, LANES)
    covariance = covariance.transpose(0, 1, 3, 2, 4).reshape(half, subs, 2, DOF * DOF)

    out_type = jax.ShapeDtypeStruct((subs, PULSES, gates), f32)
    matched_stat, power_map = pl.pallas_call(
        functools.partial(final_kernel, float(subs * n_chan * PULSES * gates * n_rng), n_rng),
        out_shape=[out_type, out_type],
        in_specs=[SMEM, VMEM, VMEM, VMEM],
        out_specs=[VMEM] * 2,
        compiler_params=params(8),
        cost_estimate=cost(1 << 20, 1 << 20),
        name="final",
    )(block, power, near_weights, stats)
    return (covariance, matched_stat, power_map)


def solution(mesh):
    placed = (
        P(None, "chan", None, "rng"),
        P("chan"),
        P("rng"),
        P("rng"),
        P(None, "chan", None, None),
    )

    return jax.shard_map(
        local,
        mesh=mesh,
        in_specs=placed,
        out_specs=(P("rng", "chan", None, None), P("chan", None, "rng"), P("chan", None, "rng")),
        check_vma=False,
    )
```

```python
import functools
import math

import jax
import jax.numpy as jnp
import numpy as np
from jax import lax
from jax.experimental import pallas as pl
from jax.experimental.pallas import tpu as pltpu
from jax.sharding import PartitionSpec as P

PULSES = 64
SUB_LEN = 32
SPAN = 8
DOF = 96
SHIFTS = DOF // SUB_LEN
LANES = 128
COV_CALLS = 1

diag_load = 1.0
f32 = jnp.float32
bf16 = jnp.bfloat16
VMEM = pl.BlockSpec(memory_space=pltpu.VMEM)
SMEM = pl.BlockSpec(memory_space=pltpu.SMEM)
HBM = pl.BlockSpec(memory_space=pltpu.HBM)
ANY = pl.BlockSpec(memory_space=pl.ANY)
BOTH = ("chan", "rng")


def params(mib, steps=0):
    semantics = ("arbitrary",) * steps if steps else None
    return pltpu.CompilerParams(vmem_limit_bytes=mib << 20, dimension_semantics=semantics)


def cost(flops, moved):
    return pl.CostEstimate(flops=int(flops), bytes_accessed=int(moved), transcendentals=0)


def in_hbm(x):
    return pltpu.with_memory_space_constraint(x, pltpu.HBM)


def dot(a, b):
    return jnp.dot(a, b, preferred_element_type=f32)


def dot_nt(a, b):
    return lax.dot_general(a, b, (((1,), (1,)), ((), ())), preferred_element_type=f32)


def dft_table(pulses):
    freq = np.arange(pulses)
    angle = 2.0 * math.pi * (freq[:, None] * freq[None, :] % pulses) / pulses
    cosine = np.cos(angle) / math.sqrt(pulses)
    sine = np.sin(angle) / math.sqrt(pulses)
    return np.block([[cosine, sine], [-sine, cosine]]).astype(np.float32)


def spectra_kernel(table_hbm, cube_hbm, *refs):
    chunks = 2
    table_ref, cube_ref, turned_re, turned_im, sems = refs[-5:]
    staged = len(refs[:-5]) // 2
    small_hbm, spec_ref, small_refs = refs[:staged], refs[staged], refs[staged + 1 : -5]
    chans, gates = cube_ref.shape[1], cube_ref.shape[3]
    each = chans // chunks
    first = pltpu.make_async_copy(table_hbm, table_ref, sems.at[chunks])
    large = [
        pltpu.make_async_copy(
            cube_hbm.at[:, pl.ds(i * each, each)], cube_ref.at[:, pl.ds(i * each, each)], sems.at[i]
        )
        for i in range(chunks)
    ]
    small = [
        pltpu.make_async_copy(src, dst, sems.at[chunks + 1 + i])
        for i, (src, dst) in enumerate(zip(small_hbm, small_refs, strict=True))
    ]
    for copy in [first, *large, *small]:
        copy.start()
    first.wait()
    table = table_ref[...]
    for c in range(0, chans, 2):
        if c % each == 0:
            large[c // each].wait()
        pair = [jnp.concatenate([cube_ref[0, e], cube_ref[1, e]], axis=0) for e in (c, c + 1)]
        out = dot(table, jnp.concatenate(pair, axis=1))
        part = c // 16
        for e in range(2):
            at = pl.ds((c + e) % 16, PULSES, stride=16)
            turned_re[part, at, :] = out[:PULSES, e * gates : (e + 1) * gates]
            turned_im[part, at, :] = out[PULSES:, e * gates : (e + 1) * gates]
        if c % 16 == 14:
            rows = slice(part * 16, part * 16 + 16)
            spec_ref[:, rows, :gates] = turned_re[part].astype(bf16).reshape(PULSES, 16, gates)
            spec_ref[:, rows, gates:] = turned_im[part].astype(bf16).reshape(PULSES, 16, gates)
    for copy in small:
        copy.wait()


def pick_kernel(halo, place_ref, index_ref, mask_ref, spec_ref, count_ref, *refs):
    refs, picked = refs[:-1], refs[-1]
    n_rng = len(refs) // 2
    full_refs, head_refs = refs[:n_rng], refs[n_rng:]
    chans, gates = spec_ref.shape[1], mask_ref.shape[1]
    train = index_ref.shape[1]
    half = PULSES // n_rng
    index = jnp.concatenate([index_ref[...], index_ref[...]], axis=1)
    row = lax.broadcasted_iota(jnp.int32, (2 * gates, 2 * train), 0)
    lane = lax.broadcasted_iota(jnp.int32, (2 * gates, 2 * train), 1)
    hit = (lax.rem(row, gates) == index) & ((row >= gates) == (lane >= train))
    select = jnp.where(hit, 1.0, 0.0).astype(bf16)
    mask = mask_ref[...].astype(f32).astype(bf16)
    mask = jnp.broadcast_to(jnp.concatenate([mask, mask], axis=1), (16, 2 * gates))
    keep = dot(mask, select)[:1]
    select = (select.astype(f32) * keep).astype(bf16)
    count_ref[...] = dot_nt(jnp.ones((8, 2 * train), bf16), select)[:, :gates]
    samples = spec_ref[...].reshape(PULSES * chans, 2 * gates)
    found = dot(samples, select).astype(bf16).reshape(PULSES, chans, 2 * train)
    picked[1 : PULSES + 1] = found
    picked[0] = found[PULSES - 1]
    picked[PULSES + 1] = found[0]
    for d in range(n_rng):
        bins = pl.ds(lax.rem(place_ref[0] + d, n_rng) * half, half + 2)
        full_refs[d][...] = picked[bins]
        head_refs[d][...] = picked[bins, :halo]


def filter_kernel(off_ref, prev_off_ref, w_ref, prev_w_ref, spec_ref, own_ref, prev_ref, banded):
    subs = w_ref.shape[1]
    chans = spec_ref.shape[1]
    gates = spec_ref.shape[2] // 2
    step = chans // subs
    per = LANES // chans
    lane = lax.broadcasted_iota(jnp.int32, (DOF, LANES), 1) & (chans - 1)
    dof = lax.broadcasted_iota(jnp.int32, (DOF, LANES), 0)
    tall = 16
    row = lax.broadcasted_iota(jnp.int32, (tall, LANES), 0)
    near = lax.broadcasted_iota(jnp.int32, (tall, LANES), 1) // chans - row
    reach = tall + 2 * per
    gaps = [near + (j - 1) * per for j in range(reach // per)]
    group = 0
    for src, (offs, taps) in enumerate(((off_ref, w_ref), (prev_off_ref, prev_w_ref))):
        for s in range(subs):
            start = src * chans - s * step - offs[:, s : s + 1]
            place = lane + start
            inside = (place >= 0) & (place < SUB_LEN)
            moves = [
                jnp.where(inside & (place + b * SUB_LEN == dof), 1.0, 0.0).astype(bf16)
                for b in range(SHIFTS)
            ]
            moves = jnp.concatenate(moves, axis=1)
            for part in range(2):
                spread = dot(taps[part, s], moves)
                for block in range(PULSES // tall):
                    before, at, after = (
                        spread[block * tall : (block + 1) * tall, b * LANES : (b + 1) * LANES]
                        for b in range(SHIFTS)
                    )
                    for j, gap in enumerate(gaps):
                        value = jnp.where(gap == 0, at, 0.0)
                        value = jnp.where(gap == -1, before, value)
                        value = jnp.where(gap == 1, after, value)
                        banded[block, group * tall : (group + 1) * tall, j * LANES : (j + 1) * LANES] = (
                            value.astype(bf16)
                        )
                group += 1
    for block in range(PULSES // tall):
        first, last = block * tall - per, (block + 1) * tall + per
        if first < 0:
            bins = [spec_ref[first + PULSES :], spec_ref[:last]]
        elif last > PULSES:
            bins = [spec_ref[first:], spec_ref[: last - PULSES]]
        else:
            bins = [spec_ref[first:last]]
        bins = [x.reshape(-1, 2 * gates) for x in bins]
        sums = dot(banded[block], jnp.concatenate(bins, axis=0))
        group = 0
        for out_ref in (own_ref, prev_ref):
            for s in range(subs):
                real = sums[group * tall : (group + 1) * tall]
                imag = sums[(group + 1) * tall : (group + 2) * tall]
                rows = slice(block * tall, (block + 1) * tall)
                out_ref[s, 0, rows, :] = real[:, :gates] + imag[:, gates:]
                out_ref[s, 1, rows, :] = real[:, gates:] - imag[:, :gates]
                group += 2


def diagonal(rows):
    return lax.broadcasted_iota(jnp.int32, (rows, LANES), 0) == (
        lax.broadcasted_iota(jnp.int32, (rows, LANES), 1) & (rows - 1)
    )


def power_kernel(train_total, own_ref, other_ref, count_ref, power_ref, stats_ref):
    subs = own_ref.shape[0]
    count = count_ref[:1] / train_total
    total = jnp.zeros((1, LANES), f32)
    quad = jnp.zeros((1, LANES), f32)
    where_sub = lax.broadcasted_iota(jnp.int32, (PULSES, LANES), 1) // PULSES
    eye = diagonal(PULSES)
    for s in range(subs):
        real = own_ref[s, 0] + other_ref[s, 0]
        imag = own_ref[s, 1] + other_ref[s, 1]
        power = real * real + imag * imag
        power_ref[s] = power
        total = total + jnp.sum(power, axis=0, keepdims=True)
        column = jnp.sum(power * count, axis=1, keepdims=True)
        quad = quad + jnp.sum(jnp.where(eye & (where_sub == s), column, 0.0), axis=0, keepdims=True)
    total = jnp.broadcast_to(jnp.sum(total, axis=1, keepdims=True), (1, LANES))
    stats_ref[...] = jnp.broadcast_to(jnp.concatenate([quad, total], axis=0)[None], stats_ref.shape)


def final_kernel(count, n_rng, block_ref, power_ref, w_ref, stats_ref, matched_ref, map_ref):
    subs = power_ref.shape[0]
    mean = jnp.sum(stats_ref[...], axis=0)[1:2] / count
    shares = jnp.sum(stats_ref[pl.ds(block_ref[0] * n_rng, n_rng)], axis=0)[:1]
    where_sub = lax.broadcasted_iota(jnp.int32, (PULSES, LANES), 1) // PULSES
    eye = diagonal(PULSES)
    for s in range(subs):
        power = power_ref[s]
        pick = jnp.where(eye & (where_sub == s), shares, 0.0)
        quad = jnp.sum(pick, axis=1, keepdims=True)
        real = w_ref[0, s].astype(f32)
        imag = w_ref[1, s].astype(f32)
        norm = jnp.sum(real * real + imag * imag, axis=1, keepdims=True)
        matched_ref[s] = power / (quad + diag_load * norm)
        map_ref[s] = power / (mean + 1e-06)


def cov_kernel(first, train_total, step, n_rng, off_ref, *refs):
    full_refs, head_refs = refs[:n_rng], refs[n_rng : 2 * n_rng]
    out_hbm, rows_scr, nat, perm, out_buf, sems = refs[-6:]
    bins, subs = out_buf.shape[0], out_buf.shape[1]
    chans, halo = full_refs[0].shape[1], head_refs[0].shape[1]
    span = chans + halo
    sign = jnp.where(
        lax.broadcasted_iota(jnp.int32, (SUB_LEN, LANES), 1) < LANES // 2, 1.0, -1.0
    )

    def prepare(i):
        for d in range(n_rng):
            rows_scr[d, pl.ds(i * span, chans), :] = full_refs[d][first + i].astype(f32)
            rows_scr[d, pl.ds(i * span + chans, halo), :] = head_refs[d][first + i].astype(f32)
        for s in range(subs):
            base = i * span + s * step + off_ref[s]
            for d in range(n_rng):
                cols = slice(d * LANES, (d + 1) * LANES)
                nat[s, i, :, cols] = rows_scr[d, pl.ds(base, SUB_LEN), :].astype(bf16)
                parts = [rows_scr[d, pl.ds(base + k, SUB_LEN // 4, stride=4), :] for k in range(4)]
                mixed = jnp.concatenate(parts, axis=0)
                perm[s, i, 0, :, cols] = mixed.astype(bf16)
                perm[s, i, 1, :, cols] = (pltpu.roll(mixed, LANES // 2, 1) * sign).astype(bf16)

    def turn(x, amount):
        x = x[:, amount // 2 * LANES : (amount // 2 + 1) * LANES]
        return pltpu.roll(x, SUB_LEN, 1) if amount % 2 else x

    def write(k):
        return pltpu.make_async_copy(
            out_buf.at[pl.ds(k, 2)], out_hbm.at[pl.ds(first + k, 2)], sems.at[k // 2]
        )

    for i in range(SHIFTS - 1):
        prepare(i)
    lane = lax.broadcasted_iota(jnp.int32, (8, LANES), 1)
    for k in range(0, bins, 2):
        prepare(k + 2)
        prepare(k + 3)
        for s in range(subs):
            right = nat[s, k : k + SHIFTS + 1].reshape((SHIFTS + 1) * SUB_LEN, n_rng * LANES)
            right = jnp.concatenate([right, right[LANES // 2 :], right[: LANES // 2]], axis=0)
            left = perm[s, k : k + SHIFTS + 1].reshape((SHIFTS + 1) * 2 * SUB_LEN, n_rng * LANES)
            prod = dot_nt(left, right) * (1.0 / train_total)
            for g in range(2):
                for b in range(SHIFTS):
                    for c in range(2):
                        at = ((b + g) * 2 + c) * SUB_LEN
                        m0, m1, m2, m3 = (
                            turn(prod[at + 8 * e : at + 8 * e + 8], (4 - e - g) % 4) for e in range(4)
                        )
                        rows = (
                            jnp.where(lane < 96, m0, m1),
                            jnp.where(lane < 64, m1, m2),
                            jnp.where(lane < 32, m2, m3),
                        )
                        for e in range(3):
                            at = 48 * b + 2 * e + c
                            out_buf[k + g, s, pl.ds(at, 8, stride=6), :] = rows[e]
        write(k).start()
    for k in range(0, bins, 2):
        write(k).wait()


def cov_scratch(bins, chans, halo, subs, n_rng):
    return [
        pltpu.VMEM((n_rng, (bins + 2) * (chans + halo), LANES), f32),
        pltpu.VMEM((subs, bins + 2, SUB_LEN, n_rng * LANES), bf16),
        pltpu.VMEM((subs, bins + 2, 2, SUB_LEN, n_rng * LANES), bf16),
        pltpu.VMEM((bins, subs, 2 * DOF * DOF // LANES, LANES), f32),
        pltpu.SemaphoreType.DMA((bins // 2,)),
    ]


def local(radar_cube, offsets, train_index, guard_mask, weights):
    n_rng = lax.axis_size("rng")
    n_chan = lax.axis_size("chan")
    subs = offsets.shape[0]
    chans, gates = radar_cube.shape[1], radar_cube.shape[3]
    train = train_index.shape[0]
    step = chans // subs
    need = (subs - 1) * step + SPAN + SUB_LEN - 1 - chans
    halo = -(-need // 8) * 8
    half = PULSES // n_rng
    train_total = train * n_rng
    samples = 2 * train

    def send(x, by_chan, by_rng):
        pairs = [
            (c * n_rng + r, (c + by_chan) % n_chan * n_rng + (r + by_rng) % n_rng)
            for c in range(n_chan)
            for r in range(n_rng)
        ]
        return lax.ppermute(x, BOTH, pairs)

    prev_weights = send(weights, 1, 0)
    prev_offsets = send(offsets, 1, 0)

    small = [
        train_index.reshape(1, train),
        guard_mask.reshape(1, gates),
        weights,
        offsets.reshape(1, subs),
    ]
    spec, near_index, near_mask, near_weights, near_offsets = pl.pallas_call(
        spectra_kernel,
        out_shape=[jax.ShapeDtypeStruct((PULSES, chans, 2 * gates), bf16)]
        + [jax.ShapeDtypeStruct(x.shape, x.dtype) for x in small],
        in_specs=[HBM] * (2 + len(small)),
        out_specs=[VMEM] * (1 + len(small)),
        scratch_shapes=[
            pltpu.VMEM((2 * PULSES, 2 * PULSES), bf16),
            pltpu.VMEM(radar_cube.shape, bf16),
            pltpu.VMEM((chans // 16, PULSES * 16, gates), f32),
            pltpu.VMEM((chans // 16, PULSES * 16, gates), f32),
            pltpu.SemaphoreType.DMA((3 + len(small),)),
        ],
        compiler_params=params(20),
        cost_estimate=cost(4 * PULSES * PULSES * chans * 2 * gates, 4 << 20),
        name="spectra",
    )(in_hbm(jnp.asarray(dft_table(PULSES), bf16)), in_hbm(radar_cube), *(in_hbm(x) for x in small))

    sums_type = jax.ShapeDtypeStruct((subs, 2, PULSES, gates), f32)
    own_sums, prev_sums = pl.pallas_call(
        filter_kernel,
        out_shape=[sums_type, sums_type],
        in_specs=[VMEM] * 5,
        out_specs=[VMEM, VMEM],
        scratch_shapes=[pltpu.VMEM((PULSES // 16, 4 * subs * 16, 16 * chans + 2 * LANES), bf16)],
        compiler_params=params(20),
        cost_estimate=cost(2 * 4 * subs * PULSES * PULSES * chans * 2 * gates, 4 << 20),
        name="filter",
    )(near_offsets, prev_offsets.reshape(1, subs), near_weights, prev_weights, spec)

    other_sums = send(prev_sums, -1, 0)
    full_type = jax.ShapeDtypeStruct((half + 2, chans, samples), bf16)
    head_type = jax.ShapeDtypeStruct((half + 2, halo, samples), bf16)
    place = lax.axis_index("rng").astype(jnp.int32).reshape(1)
    block = lax.axis_index("chan").astype(jnp.int32).reshape(1)
    count, *cut = pl.pallas_call(
        functools.partial(pick_kernel, halo),
        out_shape=[jax.ShapeDtypeStruct((8, gates), f32)] + [full_type] * n_rng + [head_type] * n_rng,
        in_specs=[SMEM, VMEM, VMEM, VMEM],
        out_specs=[VMEM] * (1 + 2 * n_rng),
        scratch_shapes=[pltpu.VMEM((PULSES + 2, chans, samples), bf16)],
        compiler_params=params(20),
        cost_estimate=cost(2 * PULSES * chans * 2 * gates * samples, 3 << 20),
        name="pick",
    )(place, near_index, near_mask, spec)
    fulls, heads = cut[:n_rng], cut[n_rng:]

    got_full = [fulls[0]]
    for d in range(1, n_rng):
        got_full.append(send(fulls[d], 0, d))

    got_head = []
    for d in range(n_rng):
        got_head.append(send(heads[d], -1, d))

    power, stats = pl.pallas_call(
        functools.partial(power_kernel, float(train_total)),
        out_shape=[
            jax.ShapeDtypeStruct((subs, PULSES, gates), f32),
            jax.ShapeDtypeStruct((n_chan * n_rng, 2, LANES), f32),
        ],
        in_specs=[VMEM] * 3,
        out_specs=[VMEM] * 2,
        compiler_params=params(8),
        cost_estimate=cost(1 << 20, 1 << 20),
        name="power",
    )(own_sums, other_sums, count)

    stats = lax.all_to_all(stats, BOTH, 0, 0, tiled=True)

    cov_type = jax.ShapeDtypeStruct((half, subs, 2 * DOF * DOF // LANES, LANES), f32)
    covariance, first = None, 0
    for part in range(COV_CALLS):
        bins = 2 * ((half // 2 * (part + 1)) // COV_CALLS) - first
        args = [near_offsets.reshape(subs), *got_full, *got_head]
        specs = [SMEM] + [VMEM] * (2 * n_rng)
        aliases = {}
        if covariance is not None:
            args.append(covariance)
            specs.append(ANY)
            aliases = {len(args) - 1: 0}
        covariance = pl.pallas_call(
            functools.partial(cov_kernel, first, float(train_total), step, n_rng),
            out_shape=cov_type,
            in_specs=specs,
            out_specs=ANY,
            scratch_shapes=cov_scratch(bins, chans, halo, subs, n_rng),
            input_output_aliases=aliases,
            compiler_params=params(20),
            cost_estimate=cost(2 * bins * subs * 192 * 128 * 256, bins * 160000),
            name="cov",
        )(*args)
        first += bins
    rows = DOF * DOF // LANES
    covariance = covariance.reshape(half, subs, rows, 2, LANES)
    covariance = covariance.transpose(0, 1, 3, 2, 4).reshape(half, subs, 2, DOF * DOF)

    out_type = jax.ShapeDtypeStruct((subs, PULSES, gates), f32)
    matched_stat, power_map = pl.pallas_call(
        functools.partial(final_kernel, float(subs * n_chan * PULSES * gates * n_rng), n_rng),
        out_shape=[out_type, out_type],
        in_specs=[SMEM, VMEM, VMEM, VMEM],
        out_specs=[VMEM] * 2,
        compiler_params=params(8),
        cost_estimate=cost(1 << 20, 1 << 20),
        name="final",
    )(block, power, near_weights, stats)
    return (covariance, matched_stat, power_map)


def solution(mesh):
    placed = (
        P(None, "chan", None, "rng"),
        P("chan"),
        P("rng"),
        P("rng"),
        P(None, "chan", None, None),
    )

    return jax.shard_map(
        local,
        mesh=mesh,
        in_specs=placed,
        out_specs=(P("rng", "chan", None, None), P("chan", None, "rng"), P("chan", None, "rng")),
        check_vma=False,
    )
```

```python
import functools
import math

import jax
import jax.numpy as jnp
import numpy as np
from jax import lax
from jax.experimental import pallas as pl
from jax.experimental.pallas import tpu as pltpu
from jax.sharding import PartitionSpec as P

PULSES = 64
SUB_LEN = 32
SPAN = 8
DOF = 96
SHIFTS = DOF // SUB_LEN
LANES = 128
COV_CALLS = 1

diag_load = 1.0
f32 = jnp.float32
bf16 = jnp.bfloat16
VMEM = pl.BlockSpec(memory_space=pltpu.VMEM)
SMEM = pl.BlockSpec(memory_space=pltpu.SMEM)
HBM = pl.BlockSpec(memory_space=pltpu.HBM)
ANY = pl.BlockSpec(memory_space=pl.ANY)
BOTH = ("chan", "rng")


def params(mib, steps=0):
    semantics = ("arbitrary",) * steps if steps else None
    return pltpu.CompilerParams(vmem_limit_bytes=mib << 20, dimension_semantics=semantics)


def cost(flops, moved):
    return pl.CostEstimate(flops=int(flops), bytes_accessed=int(moved), transcendentals=0)


def in_hbm(x):
    return pltpu.with_memory_space_constraint(x, pltpu.HBM)


def dot(a, b):
    return jnp.dot(a, b, preferred_element_type=f32)


def dot_nt(a, b):
    return lax.dot_general(a, b, (((1,), (1,)), ((), ())), preferred_element_type=f32)


def dft_table(pulses):
    freq = np.arange(pulses)
    angle = 2.0 * math.pi * (freq[:, None] * freq[None, :] % pulses) / pulses
    cosine = np.cos(angle) / math.sqrt(pulses)
    sine = np.sin(angle) / math.sqrt(pulses)
    return np.block([[cosine, sine], [-sine, cosine]]).astype(np.float32)


def spectra_kernel(table_hbm, cube_hbm, *refs):
    chunks = 2
    table_ref, cube_ref, turned_re, turned_im, sems = refs[-5:]
    staged = len(refs[:-5]) // 2
    small_hbm, spec_ref, small_refs = refs[:staged], refs[staged], refs[staged + 1 : -5]
    chans, gates = cube_ref.shape[1], cube_ref.shape[3]
    each = chans // chunks
    first = pltpu.make_async_copy(table_hbm, table_ref, sems.at[chunks])
    large = [
        pltpu.make_async_copy(
            cube_hbm.at[:, pl.ds(i * each, each)], cube_ref.at[:, pl.ds(i * each, each)], sems.at[i]
        )
        for i in range(chunks)
    ]
    small = [
        pltpu.make_async_copy(src, dst, sems.at[chunks + 1 + i])
        for i, (src, dst) in enumerate(zip(small_hbm, small_refs, strict=True))
    ]
    for copy in [first, *large, *small]:
        copy.start()
    first.wait()
    table = table_ref[...]
    for c in range(0, chans, 2):
        if c % each == 0:
            large[c // each].wait()
        pair = [jnp.concatenate([cube_ref[0, e], cube_ref[1, e]], axis=0) for e in (c, c + 1)]
        out = dot(table, jnp.concatenate(pair, axis=1))
        part = c // 16
        for e in range(2):
            at = pl.ds((c + e) % 16, PULSES, stride=16)
            turned_re[part, at, :] = out[:PULSES, e * gates : (e + 1) * gates]
            turned_im[part, at, :] = out[PULSES:, e * gates : (e + 1) * gates]
        if c % 16 == 14:
            rows = slice(part * 16, part * 16 + 16)
            spec_ref[:, rows, :gates] = turned_re[part].astype(bf16).reshape(PULSES, 16, gates)
            spec_ref[:, rows, gates:] = turned_im[part].astype(bf16).reshape(PULSES, 16, gates)
    for copy in small:
        copy.wait()


def pick_kernel(halo, place_ref, index_ref, mask_ref, spec_ref, count_ref, *refs):
    refs, picked = refs[:-1], refs[-1]
    n_rng = len(refs) // 2
    full_refs, head_refs = refs[:n_rng], refs[n_rng:]
    chans, gates = spec_ref.shape[1], mask_ref.shape[1]
    train = index_ref.shape[1]
    half = PULSES // n_rng
    index = jnp.concatenate([index_ref[...], index_ref[...]], axis=1)
    row = lax.broadcasted_iota(jnp.int32, (2 * gates, 2 * train), 0)
    lane = lax.broadcasted_iota(jnp.int32, (2 * gates, 2 * train), 1)
    hit = (lax.rem(row, gates) == index) & ((row >= gates) == (lane >= train))
    select = jnp.where(hit, 1.0, 0.0).astype(bf16)
    mask = mask_ref[...].astype(f32).astype(bf16)
    mask = jnp.broadcast_to(jnp.concatenate([mask, mask], axis=1), (16, 2 * gates))
    keep = dot(mask, select)[:1]
    select = (select.astype(f32) * keep).astype(bf16)
    count_ref[...] = dot_nt(jnp.ones((8, 2 * train), bf16), select)[:, :gates]
    samples = spec_ref[...].reshape(PULSES * chans, 2 * gates)
    found = dot(samples, select).astype(bf16).reshape(PULSES, chans, 2 * train)
    picked[1 : PULSES + 1] = found
    picked[0] = found[PULSES - 1]
    picked[PULSES + 1] = found[0]
    for d in range(n_rng):
        bins = pl.ds(lax.rem(place_ref[0] + d, n_rng) * half, half + 2)
        full_refs[d][...] = picked[bins]
        head_refs[d][...] = picked[bins, :halo]


def filter_kernel(behind, off_ref, w_ref, spec_ref, out_ref, banded):
    subs = w_ref.shape[1]
    chans = spec_ref.shape[1]
    gates = spec_ref.shape[2] // 2
    step = chans // subs
    per = LANES // chans
    lane = lax.broadcasted_iota(jnp.int32, (DOF, LANES), 1) & (chans - 1)
    dof = lax.broadcasted_iota(jnp.int32, (DOF, LANES), 0)
    tall = 16
    row = lax.broadcasted_iota(jnp.int32, (tall, LANES), 0)
    near = lax.broadcasted_iota(jnp.int32, (tall, LANES), 1) // chans - row
    reach = tall + 2 * per
    gaps = [near + (j - 1) * per for j in range(reach // per)]
    group = 0
    for s in range(subs):
        start = behind * chans - s * step - off_ref[:, s : s + 1]
        place = lane + start
        inside = (place >= 0) & (place < SUB_LEN)
        moves = [
            jnp.where(inside & (place + b * SUB_LEN == dof), 1.0, 0.0).astype(bf16)
            for b in range(SHIFTS)
        ]
        moves = jnp.concatenate(moves, axis=1)
        both = dot(jnp.concatenate([w_ref[0, s], w_ref[1, s]], axis=0), moves)
        for part in range(2):
            spread = both[part * PULSES : (part + 1) * PULSES]
            for block in range(PULSES // tall):
                before, at, after = (
                    spread[block * tall : (block + 1) * tall, b * LANES : (b + 1) * LANES]
                    for b in range(SHIFTS)
                )
                for j, gap in enumerate(gaps):
                    value = jnp.where(gap == 0, at, 0.0)
                    value = jnp.where(gap == -1, before, value)
                    value = jnp.where(gap == 1, after, value)
                    banded[block, group * tall : (group + 1) * tall, j * LANES : (j + 1) * LANES] = (
                        value.astype(bf16)
                    )
            group += 1
    for block in range(PULSES // tall):
        first, last = block * tall - per, (block + 1) * tall + per
        if first < 0:
            bins = [spec_ref[first + PULSES :], spec_ref[:last]]
        elif last > PULSES:
            bins = [spec_ref[first:], spec_ref[: last - PULSES]]
        else:
            bins = [spec_ref[first:last]]
        bins = [x.reshape(-1, 2 * gates) for x in bins]
        sums = dot(banded[block], jnp.concatenate(bins, axis=0))
        group = 0
        for s in range(subs):
            real = sums[group * tall : (group + 1) * tall]
            imag = sums[(group + 1) * tall : (group + 2) * tall]
            rows = slice(block * tall, (block + 1) * tall)
            out_ref[s, 0, rows, :] = real[:, :gates] + imag[:, gates:]
            out_ref[s, 1, rows, :] = real[:, gates:] - imag[:, :gates]
            group += 2


def diagonal(rows):
    return lax.broadcasted_iota(jnp.int32, (rows, LANES), 0) == (
        lax.broadcasted_iota(jnp.int32, (rows, LANES), 1) & (rows - 1)
    )


def power_kernel(train_total, own_ref, other_ref, count_ref, power_ref, stats_ref):
    subs = own_ref.shape[0]
    count = count_ref[:1] / train_total
    total = jnp.zeros((1, LANES), f32)
    quad = jnp.zeros((1, LANES), f32)
    where_sub = lax.broadcasted_iota(jnp.int32, (PULSES, LANES), 1) // PULSES
    eye = diagonal(PULSES)
    for s in range(subs):
        real = own_ref[s, 0] + other_ref[s, 0]
        imag = own_ref[s, 1] + other_ref[s, 1]
        power = real * real + imag * imag
        power_ref[s] = power
        total = total + jnp.sum(power, axis=0, keepdims=True)
        column = jnp.sum(power * count, axis=1, keepdims=True)
        quad = quad + jnp.sum(jnp.where(eye & (where_sub == s), column, 0.0), axis=0, keepdims=True)
    total = jnp.broadcast_to(jnp.sum(total, axis=1, keepdims=True), (1, LANES))
    stats_ref[...] = jnp.broadcast_to(jnp.concatenate([quad, total], axis=0)[None], stats_ref.shape)


def final_kernel(count, n_rng, block_ref, power_ref, w_ref, stats_ref, matched_ref, map_ref):
    subs = power_ref.shape[0]
    mean = jnp.sum(stats_ref[...], axis=0)[1:2] / count
    shares = jnp.sum(stats_ref[pl.ds(block_ref[0] * n_rng, n_rng)], axis=0)[:1]
    where_sub = lax.broadcasted_iota(jnp.int32, (PULSES, LANES), 1) // PULSES
    eye = diagonal(PULSES)
    for s in range(subs):
        power = power_ref[s]
        pick = jnp.where(eye & (where_sub == s), shares, 0.0)
        quad = jnp.sum(pick, axis=1, keepdims=True)
        real = w_ref[0, s].astype(f32)
        imag = w_ref[1, s].astype(f32)
        norm = jnp.sum(real * real + imag * imag, axis=1, keepdims=True)
        matched_ref[s] = power / (quad + diag_load * norm)
        map_ref[s] = power / (mean + 1e-06)


def cov_kernel(first, train_total, step, n_rng, off_ref, *refs):
    full_refs, head_refs = refs[:n_rng], refs[n_rng : 2 * n_rng]
    out_hbm, rows_scr, nat, perm, out_buf, sems = refs[-6:]
    bins, subs = out_buf.shape[0], out_buf.shape[1]
    chans, halo = full_refs[0].shape[1], head_refs[0].shape[1]
    span = chans + halo
    sign = jnp.where(
        lax.broadcasted_iota(jnp.int32, (SUB_LEN, LANES), 1) < LANES // 2, 1.0, -1.0
    )

    def prepare(i):
        for d in range(n_rng):
            rows_scr[d, pl.ds(i * span, chans), :] = full_refs[d][first + i].astype(f32)
            rows_scr[d, pl.ds(i * span + chans, halo), :] = head_refs[d][first + i].astype(f32)
        for s in range(subs):
            base = i * span + s * step + off_ref[s]
            for d in range(n_rng):
                cols = slice(d * LANES, (d + 1) * LANES)
                nat[s, i, :, cols] = rows_scr[d, pl.ds(base, SUB_LEN), :].astype(bf16)
                parts = [rows_scr[d, pl.ds(base + k, SUB_LEN // 4, stride=4), :] for k in range(4)]
                mixed = jnp.concatenate(parts, axis=0)
                perm[s, i, 0, :, cols] = mixed.astype(bf16)
                perm[s, i, 1, :, cols] = (pltpu.roll(mixed, LANES // 2, 1) * sign).astype(bf16)

    def turn(x, amount):
        x = x[:, amount // 2 * LANES : (amount // 2 + 1) * LANES]
        return pltpu.roll(x, SUB_LEN, 1) if amount % 2 else x

    def write(k):
        return pltpu.make_async_copy(
            out_buf.at[pl.ds(k, 2)], out_hbm.at[pl.ds(first + k, 2)], sems.at[k // 2]
        )

    for i in range(SHIFTS - 1):
        prepare(i)
    lane = lax.broadcasted_iota(jnp.int32, (8, LANES), 1)
    for k in range(0, bins, 2):
        prepare(k + 2)
        prepare(k + 3)
        for s in range(subs):
            right = nat[s, k : k + SHIFTS + 1].reshape((SHIFTS + 1) * SUB_LEN, n_rng * LANES)
            right = jnp.concatenate([right, right[LANES // 2 :], right[: LANES // 2]], axis=0)
            left = perm[s, k : k + SHIFTS + 1].reshape((SHIFTS + 1) * 2 * SUB_LEN, n_rng * LANES)
            prod = dot_nt(left, right) * (1.0 / train_total)
            for g in range(2):
                for b in range(SHIFTS):
                    for c in range(2):
                        at = ((b + g) * 2 + c) * SUB_LEN
                        m0, m1, m2, m3 = (
                            turn(prod[at + 8 * e : at + 8 * e + 8], (4 - e - g) % 4) for e in range(4)
                        )
                        rows = (
                            jnp.where(lane < 96, m0, m1),
                            jnp.where(lane < 64, m1, m2),
                            jnp.where(lane < 32, m2, m3),
                        )
                        for e in range(3):
                            at = 48 * b + 2 * e + c
                            out_buf[k + g, s, pl.ds(at, 8, stride=6), :] = rows[e]
        write(k).start()
    for k in range(0, bins, 2):
        write(k).wait()


def cov_scratch(bins, chans, halo, subs, n_rng):
    return [
        pltpu.VMEM((n_rng, (bins + 2) * (chans + halo), LANES), f32),
        pltpu.VMEM((subs, bins + 2, SUB_LEN, n_rng * LANES), bf16),
        pltpu.VMEM((subs, bins + 2, 2, SUB_LEN, n_rng * LANES), bf16),
        pltpu.VMEM((bins, subs, 2 * DOF * DOF // LANES, LANES), f32),
        pltpu.SemaphoreType.DMA((bins // 2,)),
    ]


def local(radar_cube, offsets, train_index, guard_mask, weights):
    n_rng = lax.axis_size("rng")
    n_chan = lax.axis_size("chan")
    subs = offsets.shape[0]
    chans, gates = radar_cube.shape[1], radar_cube.shape[3]
    train = train_index.shape[0]
    step = chans // subs
    need = (subs - 1) * step + SPAN + SUB_LEN - 1 - chans
    halo = -(-need // 8) * 8
    half = PULSES // n_rng
    train_total = train * n_rng
    samples = 2 * train

    def send(x, by_chan, by_rng):
        pairs = [
            (c * n_rng + r, (c + by_chan) % n_chan * n_rng + (r + by_rng) % n_rng)
            for c in range(n_chan)
            for r in range(n_rng)
        ]
        return lax.ppermute(x, BOTH, pairs)

    prev_weights = send(weights, 1, 0)
    prev_offsets = send(offsets, 1, 0)

    small = [
        train_index.reshape(1, train),
        guard_mask.reshape(1, gates),
        weights,
        offsets.reshape(1, subs),
    ]
    spec, near_index, near_mask, near_weights, near_offsets = pl.pallas_call(
        spectra_kernel,
        out_shape=[jax.ShapeDtypeStruct((PULSES, chans, 2 * gates), bf16)]
        + [jax.ShapeDtypeStruct(x.shape, x.dtype) for x in small],
        in_specs=[HBM] * (2 + len(small)),
        out_specs=[VMEM] * (1 + len(small)),
        scratch_shapes=[
            pltpu.VMEM((2 * PULSES, 2 * PULSES), bf16),
            pltpu.VMEM(radar_cube.shape, bf16),
            pltpu.VMEM((chans // 16, PULSES * 16, gates), f32),
            pltpu.VMEM((chans // 16, PULSES * 16, gates), f32),
            pltpu.SemaphoreType.DMA((3 + len(small),)),
        ],
        compiler_params=params(20),
        cost_estimate=cost(4 * PULSES * PULSES * chans * 2 * gates, 4 << 20),
        name="spectra",
    )(in_hbm(jnp.asarray(dft_table(PULSES), bf16)), in_hbm(radar_cube), *(in_hbm(x) for x in small))

    sums_type = jax.ShapeDtypeStruct((subs, 2, PULSES, gates), f32)

    def filtered(behind, offs, taps):
        return pl.pallas_call(
            functools.partial(filter_kernel, behind),
            out_shape=sums_type,
            in_specs=[VMEM] * 3,
            out_specs=VMEM,
            scratch_shapes=[
                pltpu.VMEM((PULSES // 16, 2 * subs * 16, 16 * chans + 2 * LANES), bf16)
            ],
            compiler_params=params(20),
            cost_estimate=cost(4 * subs * PULSES * PULSES * chans * 2 * gates, 3 << 20),
            name="filter",
        )(offs, taps, spec)

    own_sums = filtered(0, near_offsets, near_weights)
    prev_sums = filtered(1, prev_offsets.reshape(1, subs), prev_weights)

    other_sums = send(prev_sums, -1, 0)
    full_type = jax.ShapeDtypeStruct((half + 2, chans, samples), bf16)
    head_type = jax.ShapeDtypeStruct((half + 2, halo, samples), bf16)
    place = lax.axis_index("rng").astype(jnp.int32).reshape(1)
    block = lax.axis_index("chan").astype(jnp.int32).reshape(1)
    count, *cut = pl.pallas_call(
        functools.partial(pick_kernel, halo),
        out_shape=[jax.ShapeDtypeStruct((8, gates), f32)] + [full_type] * n_rng + [head_type] * n_rng,
        in_specs=[SMEM, VMEM, VMEM, VMEM],
        out_specs=[VMEM] * (1 + 2 * n_rng),
        scratch_shapes=[pltpu.VMEM((PULSES + 2, chans, samples), bf16)],
        compiler_params=params(20),
        cost_estimate=cost(2 * PULSES * chans * 2 * gates * samples, 3 << 20),
        name="pick",
    )(place, near_index, near_mask, spec)
    fulls, heads = cut[:n_rng], cut[n_rng:]

    got_full = [fulls[0]]
    for d in range(1, n_rng):
        got_full.append(send(fulls[d], 0, d))

    got_head = []
    for d in range(n_rng):
        got_head.append(send(heads[d], -1, d))

    power, stats = pl.pallas_call(
        functools.partial(power_kernel, float(train_total)),
        out_shape=[
            jax.ShapeDtypeStruct((subs, PULSES, gates), f32),
            jax.ShapeDtypeStruct((n_chan * n_rng, 2, LANES), f32),
        ],
        in_specs=[VMEM] * 3,
        out_specs=[VMEM] * 2,
        compiler_params=params(8),
        cost_estimate=cost(1 << 20, 1 << 20),
        name="power",
    )(own_sums, other_sums, count)

    stats = lax.all_to_all(stats, BOTH, 0, 0, tiled=True)

    cov_type = jax.ShapeDtypeStruct((half, subs, 2 * DOF * DOF // LANES, LANES), f32)
    covariance, first = None, 0
    for part in range(COV_CALLS):
        bins = 2 * ((half // 2 * (part + 1)) // COV_CALLS) - first
        args = [near_offsets.reshape(subs), *got_full, *got_head]
        specs = [SMEM] + [VMEM] * (2 * n_rng)
        aliases = {}
        if covariance is not None:
            args.append(covariance)
            specs.append(ANY)
            aliases = {len(args) - 1: 0}
        covariance = pl.pallas_call(
            functools.partial(cov_kernel, first, float(train_total), step, n_rng),
            out_shape=cov_type,
            in_specs=specs,
            out_specs=ANY,
            scratch_shapes=cov_scratch(bins, chans, halo, subs, n_rng),
            input_output_aliases=aliases,
            compiler_params=params(20),
            cost_estimate=cost(2 * bins * subs * 192 * 128 * 256, bins * 160000),
            name="cov",
        )(*args)
        first += bins
    rows = DOF * DOF // LANES
    covariance = covariance.reshape(half, subs, rows, 2, LANES)
    covariance = covariance.transpose(0, 1, 3, 2, 4).reshape(half, subs, 2, DOF * DOF)

    out_type = jax.ShapeDtypeStruct((subs, PULSES, gates), f32)
    matched_stat, power_map = pl.pallas_call(
        functools.partial(final_kernel, float(subs * n_chan * PULSES * gates * n_rng), n_rng),
        out_shape=[out_type, out_type],
        in_specs=[SMEM, VMEM, VMEM, VMEM],
        out_specs=[VMEM] * 2,
        compiler_params=params(8),
        cost_estimate=cost(1 << 20, 1 << 20),
        name="final",
    )(block, power, near_weights, stats)
    return (covariance, matched_stat, power_map)


def solution(mesh):
    placed = (
        P(None, "chan", None, "rng"),
        P("chan"),
        P("rng"),
        P("rng"),
        P(None, "chan", None, None),
    )

    return jax.shard_map(
        local,
        mesh=mesh,
        in_specs=placed,
        out_specs=(P("rng", "chan", None, None), P("chan", None, "rng"), P("chan", None, "rng")),
        check_vma=False,
    )
```
